32 devices in a mesh: ctx: 8 (over z, core), fsdp: 4 (over y, x).
Axes of the slice: x: 2, y: 2, z: 4, core: 2. Of those that a mesh axis runs over, the one named last changes fastest.
Arguments:
- inputs: float32 [4096, 2048], P(('ctx', 'fsdp')), may hold values from -6 to 6
- cotangent: float32 [4096, 2048], P(('ctx', 'fsdp')), may hold values from -6 to 6
- positions: int32 [4096], replicated, may hold values from 0 to 4095, as said below
- gain_attention: float32 [2048], P('ctx'), may hold values from 0.9 to 1.1
- shift_attention: float32 [2048], P('ctx'), may hold values from -0.18 to 0.18
- weight_project: float32 [2048, 3, 2048], P('ctx', None, 'fsdp'), may hold values from -0.1875 to 0.1875
- bias_project: float32 [3, 32, 64], P(None, 'fsdp', 'ctx'), may hold values from -0.18 to 0.18
- weight_output: float32 [2048, 2048], P('fsdp', 'ctx'), may hold values from -0.75 to 0.75
- gain_feedforward: float32 [2048], P('ctx'), may hold values from 0.1 to 1.9
- shift_feedforward: float32 [2048], P('ctx'), may hold values from -0.18 to 0.18
- weight_gateup: float32 [2048, 2, 5632], P('ctx', None, 'fsdp'), may hold values from -0.125 to 0.125
- weight_down: float32 [5632, 2048], P('fsdp', 'ctx'), may hold values from -0.078125 to 0.078125
- momentum_gain_attention: float32 [2048], P('ctx'), may hold values from -20 to 20
- momentum_shift_attention: float32 [2048], P('ctx'), may hold values from -20 to 20
- momentum_weight_project: float32 [2048, 3, 2048], P('ctx', None, 'fsdp'), may hold values from -20 to 20
- momentum_bias_project: float32 [3, 32, 64], P(None, 'fsdp', 'ctx'), may hold values from -20 to 20
- momentum_weight_output: float32 [2048, 2048], P('fsdp', 'ctx'), may hold values from -20 to 20
- momentum_gain_feedforward: float32 [2048], P('ctx'), may hold values from -20 to 20
- momentum_shift_feedforward: float32 [2048], P('ctx'), may hold values from -20 to 20
- momentum_weight_gateup: float32 [2048, 2, 5632], P('ctx', None, 'fsdp'), may hold values from -20 to 20
- momentum_weight_down: float32 [5632, 2048], P('fsdp', 'ctx'), may hold values from -20 to 20
- variance_gain_attention: float32 [2048], P('ctx'), may hold values from 409.6 to 1638.4
- variance_shift_attention: float32 [2048], P('ctx'), may hold values from 409.6 to 1638.4
- variance_weight_project: float32 [2048, 3, 2048], P('ctx', None, 'fsdp'), may hold values from 40.96 to 163.84
- variance_bias_project: float32 [3, 32, 64], P(None, 'fsdp', 'ctx'), may hold values from 40.96 to 163.84
- variance_weight_output: float32 [2048, 2048], P('fsdp', 'ctx'), may hold values from 40.96 to 163.84
- variance_gain_feedforward: float32 [2048], P('ctx'), may hold values from 40.96 to 163.84
- variance_shift_feedforward: float32 [2048], P('ctx'), may hold values from 40.96 to 163.84
- variance_weight_gateup: float32 [2048, 2, 5632], P('ctx', None, 'fsdp'), may hold values from 40.96 to 163.84
- variance_weight_down: float32 [5632, 2048], P('fsdp', 'ctx'), may hold values from 40.96 to 163.84
Outputs:
- output: float32 [4096, 2048], P(('ctx', 'fsdp'))
- input_grad: float32 [4096, 2048], P(('ctx', 'fsdp'))
- gradient_gain_attention: float32 [2048], P('ctx')
- gradient_shift_attention: float32 [2048], P('ctx')
- gradient_weight_project: float32 [2048, 3, 2048], P('ctx', None, 'fsdp')
- gradient_bias_project: float32 [3, 32, 64], P(None, 'fsdp', 'ctx')
- gradient_weight_output: float32 [2048, 2048], P('fsdp', 'ctx')
- gradient_gain_feedforward: float32 [2048], P('ctx')
- gradient_shift_feedforward: float32 [2048], P('ctx')
- gradient_weight_gateup: float32 [2048, 2, 5632], P('ctx', None, 'fsdp')
- gradient_weight_down: float32 [5632, 2048], P('fsdp', 'ctx')
- update_gain_attention: float32 [2048], P('ctx')
- new_shift_attention: float32 [2048], P('ctx')
- new_weight_project: float32 [2048, 3, 2048], P('ctx', None, 'fsdp')
- new_bias_project: float32 [3, 32, 64], P(None, 'fsdp', 'ctx')
- new_weight_output: float32 [2048, 2048], P('fsdp', 'ctx')
- update_gain_feedforward: float32 [2048], P('ctx')
- new_shift_feedforward: float32 [2048], P('ctx')
- new_weight_gateup: float32 [2048, 2, 5632], P('ctx', None, 'fsdp')
- new_weight_down: float32 [5632, 2048], P('fsdp', 'ctx')
- next_momentum_gain_attention: float32 [2048], P('ctx')
- next_momentum_shift_attention: float32 [2048], P('ctx')
- next_momentum_weight_project: float32 [2048, 3, 2048], P('ctx', None, 'fsdp')
- next_momentum_bias_project: float32 [3, 32, 64], P(None, 'fsdp', 'ctx')
- next_momentum_weight_output: float32 [2048, 2048], P('fsdp', 'ctx')
- next_momentum_gain_feedforward: float32 [2048], P('ctx')
- next_momentum_shift_feedforward: float32 [2048], P('ctx')
- next_momentum_weight_gateup: float32 [2048, 2, 5632], P('ctx', None, 'fsdp')
- next_momentum_weight_down: float32 [5632, 2048], P('fsdp', 'ctx')
- next_variance_gain_attention: float32 [2048], P('ctx')
- next_variance_shift_attention: float32 [2048], P('ctx')
- next_variance_weight_project: float32 [2048, 3, 2048], P('ctx', None, 'fsdp')
- next_variance_bias_project: float32 [3, 32, 64], P(None, 'fsdp', 'ctx')
- next_variance_weight_output: float32 [2048, 2048], P('fsdp', 'ctx')
- next_variance_gain_feedforward: float32 [2048], P('ctx')
- next_variance_shift_feedforward: float32 [2048], P('ctx')
- next_variance_weight_gateup: float32 [2048, 2, 5632], P('ctx', None, 'fsdp')
- next_variance_weight_down: float32 [5632, 2048], P('fsdp', 'ctx')
The draws below stay inside these ranges and needn't reach their ends.
Inputs may be any that keep to these rules, and one draw needn't show every extreme that they name: positions holds each of 0 to 4095 once. Rows fall in aligned runs of 256, each holding one block of 256 consecutive positions in rising order, and the two runs of each aligned run of 512 rows hold block j and block 15 - j for some j.
All inputs are finite; a program needn't handle non-finite values.
Results may differ from the reference program's by a relative error of at most 0.025.
Values may be sent and summed in bfloat16 or wider, within the bound.
A program may use at most 160 MiB of HBM per device.

```python
import math
from functools import partial
import jax
import jax.numpy as jnp
from jax import lax

D = 2048
H = 32
HD = 64
ROT = 16
FF = 5632
SEQ = 4096
BLK = 256


def draw_positions(key, part):
    pair_count = SEQ // (2 * BLK)
    pair_order = jax.random.permutation(jax.random.fold_in(key, 11), pair_count)
    flip_bits = jax.random.randint(jax.random.fold_in(key, 12), (pair_count,), 0, 2)
    first_block = jnp.where(flip_bits == 0, pair_order, 2 * pair_count - 1 - pair_order)
    second_block = 2 * pair_count - 1 - first_block
    block_ids = jnp.stack([first_block, second_block], axis=1).reshape(-1)
    return (block_ids[:, None] * BLK + jnp.arange(BLK, dtype=jnp.int32)[None, :]).reshape(-1).astype(jnp.int32)


def block_levels(rng, shape, pieces, smallest, largest):
    gain, own = 1.0, jax.random.fold_in(rng, 6)
    for position, parts in pieces:
        draws = jnp.exp(jax.random.uniform(jax.random.fold_in(own, position), (parts,), jnp.float32, smallest / len(pieces), largest / len(pieces)))
        gain = gain * jnp.repeat(draws, shape[position] // parts).reshape([-1 if axis == position else 1 for axis in range(len(shape))])
    return gain


def bell_draw(rng, dims, scale, reach, shards=(), kind=jnp.bfloat16):
    array = jax.random.normal(rng, dims, jnp.float32) * scale
    if len(shards) > 0:
        array = block_levels(rng, dims, shards, -0.22, 0.18) * array
    return jnp.clip(array, min=-reach, max=reach).astype(kind)


def setup_inputs(seed: int = 0) -> dict:
    key_of = jax.random.split(jax.random.key(seed), 31)
    inputs = bell_draw(key_of[0], (SEQ, D), 1.0, 6.0, ((0, 32),), jnp.float32)
    cotangent = bell_draw(key_of[1], (SEQ, D), 1.0, 6.0, ((0, 32),), jnp.float32)
    positions = draw_positions(jax.random.fold_in(key_of[30], 71), 0)
    gain_attention = jnp.clip(1.0 + 0.02 * jax.random.normal(key_of[3], (D,), jnp.float32), 0.9, 1.1)
    shift_attention = bell_draw(key_of[4], (D,), 0.03, 0.18, ((0, 8),), jnp.float32)
    weight_project = bell_draw(key_of[5], (D, 3, D), (D // 2) ** -0.5, 0.1875, ((0, 8), (2, 4)), jnp.float32)
    bias_project = bell_draw(key_of[6], (3, H, HD), 0.03, 0.18, ((1, 4), (2, 8)), jnp.float32)
    weight_output = bell_draw(key_of[7], (D, D), (max(1, D * 128 // SEQ)) ** -0.5, 0.75, ((0, 4), (1, 8)), jnp.float32)
    gain_feedforward = jnp.clip(1.0 + 0.18 * jax.random.normal(key_of[8], (D,), jnp.float32), 0.1, 1.9)
    shift_feedforward = bell_draw(key_of[9], (D,), 0.03, 0.18, ((0, 8),), jnp.float32)
    weight_gateup = bell_draw(key_of[10], (D, 2, FF), D ** -0.5, 0.125, ((0, 8), (2, 4)), jnp.float32)
    weight_down = bell_draw(key_of[11], (FF, D), FF ** -0.5, 0.078125, ((0, 4), (1, 8)), jnp.float32)
    momentum_gain_attention = bell_draw(key_of[12], (D,), (0.05 * SEQ ** 0.5), 20.0, ((0, 8),), jnp.float32)
    momentum_shift_attention = bell_draw(key_of[13], (D,), (0.05 * SEQ ** 0.5), 20.0, ((0, 8),), jnp.float32)
    momentum_weight_project = bell_draw(key_of[14], (D, 3, D), (0.05 * SEQ ** 0.5), 20.0, ((0, 8), (2, 4)), jnp.float32)
    momentum_bias_project = bell_draw(key_of[15], (3, H, HD), (0.05 * SEQ ** 0.5), 20.0, ((1, 4), (2, 8)), jnp.float32)
    momentum_weight_output = bell_draw(key_of[16], (D, D), (0.05 * SEQ ** 0.5), 20.0, ((0, 4), (1, 8)), jnp.float32)
    momentum_gain_feedforward = bell_draw(key_of[17], (D,), (0.05 * SEQ ** 0.5), 20.0, ((0, 8),), jnp.float32)
    momentum_shift_feedforward = bell_draw(key_of[18], (D,), (0.05 * SEQ ** 0.5), 20.0, ((0, 8),), jnp.float32)
    momentum_weight_gateup = bell_draw(key_of[19], (D, 2, FF), (0.05 * SEQ ** 0.5), 20.0, ((0, 8), (2, 4)), jnp.float32)
    momentum_weight_down = bell_draw(key_of[20], (FF, D), (0.05 * SEQ ** 0.5), 20.0, ((0, 4), (1, 8)), jnp.float32)
    variance_gain_attention = jnp.clip(jnp.exp(math.log(1638.4) - 1.3862944 * jax.random.uniform(key_of[21], (D,), jnp.float32) ** block_levels(key_of[21], (D,), ((0, 8),), -0.2, 0.2)), 409.6, 1638.4)
    variance_shift_attention = jnp.clip(jnp.exp(math.log(1638.4) - 1.3862944 * jax.random.uniform(key_of[22], (D,), jnp.float32) ** block_levels(key_of[22], (D,), ((0, 8),), -0.2, 0.2)), 409.6, 1638.4)
    variance_weight_project = jnp.clip(jnp.exp(math.log(163.84) - 1.3862944 * jax.random.uniform(key_of[23], (D, 3, D), jnp.float32) ** block_levels(key_of[23], (D, 3, D), ((0, 8), (2, 4)), -0.2, 0.2)), 40.96, 163.84)
    variance_bias_project = jnp.clip(jnp.exp(math.log(163.84) - 1.3862944 * jax.random.uniform(key_of[24], (3, H, HD), jnp.float32) ** block_levels(key_of[24], (3, H, HD), ((1, 4), (2, 8)), -0.2, 0.2)), 40.96, 163.84)
    variance_weight_output = jnp.clip(jnp.exp(math.log(163.84) - 1.3862944 * jax.random.uniform(key_of[25], (D, D), jnp.float32) ** block_levels(key_of[25], (D, D), ((0, 4), (1, 8)), -0.2, 0.2)), 40.96, 163.84)
    variance_gain_feedforward = jnp.clip(jnp.exp(math.log(163.84) - 1.3862944 * jax.random.uniform(key_of[26], (D,), jnp.float32) ** block_levels(key_of[26], (D,), ((0, 8),), -0.2, 0.2)), 40.96, 163.84)
    variance_shift_feedforward = jnp.clip(jnp.exp(math.log(163.84) - 1.3862944 * jax.random.uniform(key_of[27], (D,), jnp.float32) ** block_levels(key_of[27], (D,), ((0, 8),), -0.2, 0.2)), 40.96, 163.84)
    variance_weight_gateup = jnp.clip(jnp.exp(math.log(163.84) - 1.3862944 * jax.random.uniform(key_of[28], (D, 2, FF), jnp.float32) ** block_levels(key_of[28], (D, 2, FF), ((0, 8), (2, 4)), -0.2, 0.2)), 40.96, 163.84)
    variance_weight_down = jnp.clip(jnp.exp(math.log(163.84) - 1.3862944 * jax.random.uniform(key_of[29], (FF, D), jnp.float32) ** block_levels(key_of[29], (FF, D), ((0, 4), (1, 8)), -0.2, 0.2)), 40.96, 163.84)
    return {"inputs": inputs, "cotangent": cotangent, "positions": positions, "gain_attention": gain_attention, "shift_attention": shift_attention, "weight_project": weight_project, "bias_project": bias_project, "weight_output": weight_output, "gain_feedforward": gain_feedforward, "shift_feedforward": shift_feedforward, "weight_gateup": weight_gateup, "weight_down": weight_down, "momentum_gain_attention": momentum_gain_attention, "momentum_shift_attention": momentum_shift_attention, "momentum_weight_project": momentum_weight_project, "momentum_bias_project": momentum_bias_project, "momentum_weight_output": momentum_weight_output, "momentum_gain_feedforward": momentum_gain_feedforward, "momentum_shift_feedforward": momentum_shift_feedforward, "momentum_weight_gateup": momentum_weight_gateup, "momentum_weight_down": momentum_weight_down, "variance_gain_attention": variance_gain_attention, "variance_shift_attention": variance_shift_attention, "variance_weight_project": variance_weight_project, "variance_bias_project": variance_bias_project, "variance_weight_output": variance_weight_output, "variance_gain_feedforward": variance_gain_feedforward, "variance_shift_feedforward": variance_shift_feedforward, "variance_weight_gateup": variance_weight_gateup, "variance_weight_down": variance_weight_down}


@jax.custom_vjp
def low(v):
    return lax.optimization_barrier(v.astype(jnp.bfloat16)).astype(jnp.float32)

@jax.custom_vjp
def low_back(v):
    return v

def low_keep(v):
    return (low(v), None)

def low_pass(kept, grad):
    return (grad,)

def back_keep(v):
    return (v, None)

def back_low(kept, grad):
    return (low(grad),)
low.defvjp(low_keep, low_pass)
low_back.defvjp(back_keep, back_low)
norm_eps = 1e-05
rope_base = 10000.0
masked_score = -1e+30
learn_rate = 0.1
beta_one = 0.9
beta_two = 0.95
adam_eps = 1e-08
decay_rate = 0.1
adam_step = 10
highest_precision = lax.Precision.HIGHEST

def norm_apply(values, gain_vector, shift_vector):
    center = values - lax.optimization_barrier(jnp.mean(values, axis=-1, keepdims=True))
    inverse = lax.rsqrt(lax.optimization_barrier(jnp.mean(center * center, axis=-1, keepdims=True)) + norm_eps)
    return center * inverse * gain_vector + shift_vector

def rotate(head_values, where_at):
    half_dims = ROT // 2
    frequency = rope_base ** (-(jnp.arange(half_dims, dtype=jnp.float32) * 2.0) / ROT)
    angles = where_at.astype(jnp.float32)[:, None] * frequency[None, :]
    cosine = jnp.cos(angles)[:, None, :]
    sine_part = jnp.sin(angles)[:, None, :]
    first_half = head_values[..., :half_dims]
    second = head_values[..., half_dims:ROT]
    return jnp.concatenate([first_half * cosine - second * sine_part, second * cosine + first_half * sine_part, head_values[..., ROT:]], axis=-1)

def attend(queries, key_heads, values, where_at):
    row_count = queries.shape[0]
    block_rows = math.gcd(row_count, 512)
    score_scale = HD ** (-0.5)

    def one_block(block_item):
        query_block, query_pos = block_item
        scores = low_back(jnp.einsum('qhd,khd->hqk', query_block, key_heads, precision=highest_precision) * score_scale)
        allowed = (query_pos[:, None] >= where_at[None, :])[None]
        scores = jnp.where(allowed, scores, masked_score)
        row_top = lax.optimization_barrier(jnp.max(scores, axis=-1, keepdims=True))
        expos = jnp.exp(scores - row_top)
        weights = low(expos / lax.optimization_barrier(jnp.sum(expos, axis=-1, keepdims=True)))
        return jnp.einsum('hqk,khd->qhd', weights, values, precision=highest_precision)
    query_blocks = queries.reshape(row_count // block_rows, block_rows, H, HD)
    pos_blocks = where_at.reshape(row_count // block_rows, block_rows)
    mixed = lax.map(jax.checkpoint(one_block), (query_blocks, pos_blocks))
    return mixed.reshape(row_count, D)

def layer_forward(where_at, inputs, gain_one, shift_one, project, bias_vector, output_matrix, gain_two, shift_two, gateup, down_matrix):
    row_count = inputs.shape[0]
    project_flat = low(project).reshape(D, 3 * D)
    bias_flat = low(bias_vector).reshape(3 * D)
    gateup_flat = low(gateup).reshape(D, 2 * FF)
    first_act = low(norm_apply(inputs, low(gain_one), low(shift_one)))
    projected = low_back(jnp.dot(first_act, project_flat, precision=highest_precision, preferred_element_type=jnp.float32) + bias_flat)
    split_cols = projected.reshape(row_count, 3, H, HD)
    queries = low(low_back(rotate(split_cols[:, 0], where_at)))
    key_heads = low(low_back(rotate(split_cols[:, 1], where_at)))
    values = low(low_back(split_cols[:, 2]))
    mixed = low(low_back(attend(queries, key_heads, values, where_at)))
    middle = inputs + low_back(jnp.dot(mixed, low(output_matrix), precision=highest_precision, preferred_element_type=jnp.float32))
    second_act = low(norm_apply(middle, low(gain_two), low(shift_two)))
    gate_up = low_back(jnp.dot(second_act, gateup_flat, precision=highest_precision, preferred_element_type=jnp.float32))
    hidden = low(jax.nn.silu(gate_up[:, :FF]) * gate_up[:, FF:])
    return middle + low_back(jnp.dot(hidden, low(down_matrix), precision=highest_precision, preferred_element_type=jnp.float32))

def reference(inputs, cotangent, positions, gain_attention, shift_attention, weight_project, bias_project, weight_output, gain_feedforward, shift_feedforward, weight_gateup, weight_down, momentum_gain_attention, momentum_shift_attention, momentum_weight_project, momentum_bias_project, momentum_weight_output, momentum_gain_feedforward, momentum_shift_feedforward, momentum_weight_gateup, momentum_weight_down, variance_gain_attention, variance_shift_attention, variance_weight_project, variance_bias_project, variance_weight_output, variance_gain_feedforward, variance_shift_feedforward, variance_weight_gateup, variance_weight_down):
    params = [gain_attention, shift_attention, weight_project, bias_project, weight_output, gain_feedforward, shift_feedforward, weight_gateup, weight_down]
    momenta = [momentum_gain_attention, momentum_shift_attention, momentum_weight_project, momentum_bias_project, momentum_weight_output, momentum_gain_feedforward, momentum_shift_feedforward, momentum_weight_gateup, momentum_weight_down]
    variances = [variance_gain_attention, variance_shift_attention, variance_weight_project, variance_bias_project, variance_weight_output, variance_gain_feedforward, variance_shift_feedforward, variance_weight_gateup, variance_weight_down]
    output, pullback = jax.vjp(partial(layer_forward, positions), inputs, *params)
    gradients = pullback(cotangent)
    new_params = []
    new_momenta = []
    new_variances = []
    for index in range(9):
        grad_value = gradients[index + 1]
        moment = beta_one * momenta[index] + (1.0 - beta_one) * grad_value
        second_moment = beta_two * variances[index] + (1.0 - beta_two) * grad_value * grad_value
        corrected = moment / (1.0 - beta_one ** adam_step)
        root_term = jnp.sqrt(second_moment / (1.0 - beta_two ** adam_step)) + adam_eps
        new_params.append(params[index] - learn_rate * (corrected / root_term + decay_rate * params[index]))
        new_momenta.append(moment)
        new_variances.append(second_moment)
    update_first = new_params[0] - params[0]
    update_second = new_params[5] - params[5]
    return (output, gradients[0], gradients[1], gradients[2], gradients[3], gradients[4], gradients[5], gradients[6], gradients[7], gradients[8], gradients[9], update_first, new_params[1], new_params[2], new_params[3], new_params[4], update_second, new_params[6], new_params[7], new_params[8], new_momenta[0], new_momenta[1], new_momenta[2], new_momenta[3], new_momenta[4], new_momenta[5], new_momenta[6], new_momenta[7], new_momenta[8], new_variances[0], new_variances[1], new_variances[2], new_variances[3], new_variances[4], new_variances[5], new_variances[6], new_variances[7], new_variances[8])
```

```python
from functools import partial
import math

import jax
import jax.numpy as jnp
from jax import lax
from jax.experimental import pallas as pl
from jax.experimental.pallas import tpu as pltpu
from jax.sharding import PartitionSpec as P

D = 2048
H = 32
HD = 64
ROT = 16


norm_eps = 1e-05
rope_base = 10000.0
masked_score = -1e30
learn_rate = 0.1
beta_one = 0.9
beta_two = 0.95
adam_eps = 1e-08
decay_rate = 0.1
adam_step = 10


def norm_parts(values):
    center = values - jnp.mean(values, axis=-1, keepdims=True)
    inverse = lax.rsqrt(jnp.mean(center * center, axis=-1, keepdims=True) + norm_eps)
    return (center * inverse, inverse)


def norm_back(grad_out, normed, inverse, gain_vector):
    scaled = grad_out * gain_vector
    inner_mean = jnp.mean(scaled * normed, axis=-1, keepdims=True)
    return (scaled - jnp.mean(scaled, axis=-1, keepdims=True) - normed * inner_mean) * inverse


def keep_state(state_now):
    return state_now


def masked_scores(query_block, key_block, query_pos, key_pos):
    scores = jnp.einsum(
        "qhd,khd->hqk", query_block, key_block, preferred_element_type=jnp.float32
    ) * HD ** (-0.5)
    allowed = (query_pos[:, None] >= key_pos[None, :])[None]
    return (scores, allowed)


def attend_block(query_block, query_pos, key_sub, value_sub, pos_sub, state_now):
    row_top, row_total, weighted = state_now
    scores, allowed = masked_scores(query_block, key_sub, query_pos, pos_sub)
    scores = jnp.where(allowed, scores, masked_score)
    new_top = jnp.maximum(row_top, jnp.max(scores, axis=-1))
    weights = jnp.where(allowed, jnp.exp(scores - new_top[..., None]), 0.0)
    factor = jnp.exp(row_top - new_top)
    mixed_block = jnp.einsum(
        "hqk,khd->hqd", weights.astype(jnp.bfloat16), value_sub, preferred_element_type=jnp.float32
    )
    return (
        new_top,
        row_total * factor + jnp.sum(weights, axis=-1),
        weighted * factor[..., None] + mixed_block,
    )


def back_block(
    query_block, query_pos, grad_block, lse_half, delta_half, key_sub, value_sub, pos_sub, state_now
):
    query_grad, key_grad, value_grad = state_now
    scores, allowed = masked_scores(query_block, key_sub, query_pos, pos_sub)
    weights = jnp.where(allowed, jnp.exp(scores - lse_half[..., None]), 0.0)
    value_grad = value_grad + jnp.einsum(
        "hqk,qhd->khd", weights.astype(jnp.bfloat16), grad_block, preferred_element_type=jnp.float32
    )
    weight_grads = jnp.einsum(
        "qhd,khd->hqk", grad_block, value_sub, preferred_element_type=jnp.float32
    )
    score_grads = (weights * (weight_grads - delta_half[..., None])).astype(jnp.bfloat16)
    query_grad = query_grad + jnp.einsum(
        "hqk,khd->hqd", score_grads, key_sub, preferred_element_type=jnp.float32
    ) * HD ** (-0.5)
    key_grad = key_grad + jnp.einsum(
        "hqk,qhd->khd", score_grads, query_block, preferred_element_type=jnp.float32
    ) * HD ** (-0.5)
    return (query_grad, key_grad, value_grad)


def piece_layout(shard_piece, pos_all, row_count):
    key_piece, value_piece = shard_piece
    piece_rows = key_piece.shape[0]
    block_rows = math.gcd(piece_rows, row_count)
    block_count = piece_rows // block_rows
    key_pos = pos_all.reshape(block_count, block_rows)
    key_blocks = key_piece.reshape(block_count, block_rows, -1, HD)
    value_blocks = value_piece.reshape(block_count, block_rows, -1, HD)
    return (block_rows, block_count, key_pos, key_blocks, value_blocks)


def query_side_fold(block_fns, pos_halves, pos_all, row_count, states, shard_piece):
    block_rows, block_count, key_pos, key_blocks, value_blocks = piece_layout(
        shard_piece, pos_all, row_count
    )
    sub_rows = block_rows // 2

    def query_scan_step(carried, block_item):
        key_block, value_block, block_pos = block_item
        current = [carried[0], carried[1]]
        for key_half in range(2):
            key_sub = key_block[key_half * sub_rows : (key_half + 1) * sub_rows]
            value_sub = value_block[key_half * sub_rows : (key_half + 1) * sub_rows]
            pos_sub = block_pos[key_half * sub_rows : (key_half + 1) * sub_rows]
            for which_half in range(2):
                needed = jnp.min(pos_sub) <= jnp.max(pos_halves[which_half])
                current[which_half] = lax.cond(
                    needed,
                    partial(block_fns[which_half], key_sub, value_sub, pos_sub),
                    keep_state,
                    current[which_half],
                )
        return ((current[0], current[1]), None)

    states, unused = lax.scan(query_scan_step, states, (key_blocks, value_blocks, key_pos))
    return states


def backward_fold(
    query_halves,
    pos_halves,
    grad_halves,
    lse_halves,
    delta_halves,
    pos_all,
    row_count,
    states,
    shard_piece,
):
    block_rows, block_count, key_pos, key_blocks, value_blocks = piece_layout(
        shard_piece, pos_all, row_count
    )
    sub_rows = block_rows // 2
    offsets = jnp.arange(block_count, dtype=jnp.int32) * block_rows

    def backward_scan_step(carried, block_item):
        query_grads, key_grads, value_grads = carried
        key_block, value_block, block_pos, offset = block_item
        current = [query_grads[0], query_grads[1]]
        key_parts = []
        value_parts = []
        for key_half in range(2):
            key_sub = key_block[key_half * sub_rows : (key_half + 1) * sub_rows]
            value_sub = value_block[key_half * sub_rows : (key_half + 1) * sub_rows]
            pos_sub = block_pos[key_half * sub_rows : (key_half + 1) * sub_rows]
            key_acc = jnp.zeros((sub_rows, key_block.shape[1], HD), jnp.float32)
            value_acc = jnp.zeros((sub_rows, key_block.shape[1], HD), jnp.float32)
            for which_half in range(2):
                needed = jnp.min(pos_sub) <= jnp.max(pos_halves[which_half])
                current[which_half], key_acc, value_acc = lax.cond(
                    needed,
                    partial(
                        back_block,
                        query_halves[which_half],
                        pos_halves[which_half],
                        grad_halves[which_half],
                        lse_halves[which_half],
                        delta_halves[which_half],
                        key_sub,
                        value_sub,
                        pos_sub,
                    ),
                    keep_state,
                    (current[which_half], key_acc, value_acc),
                )
            key_parts.append(key_acc)
            value_parts.append(value_acc)
        key_grads = lax.dynamic_update_slice_in_dim(
            key_grads, jnp.concatenate(key_parts, axis=0).reshape(block_rows, -1), offset, 0
        )
        value_grads = lax.dynamic_update_slice_in_dim(
            value_grads, jnp.concatenate(value_parts, axis=0).reshape(block_rows, -1), offset, 0
        )
        return (((current[0], current[1]), key_grads, value_grads), None)

    states, unused = lax.scan(
        backward_scan_step, states, (key_blocks, value_blocks, key_pos, offsets)
    )
    return states


def adam_update(param, grad_value, moment_old, second_old):
    moment = beta_one * moment_old + (1.0 - beta_one) * grad_value
    second_moment = beta_two * second_old + (1.0 - beta_two) * grad_value * grad_value
    corrected = moment / (1.0 - beta_one**adam_step)
    root_term = jnp.sqrt(second_moment / (1.0 - beta_two**adam_step)) + adam_eps
    return (
        param - learn_rate * (corrected / root_term + decay_rate * param),
        moment,
        second_moment,
    )


F32=jnp.float32; BF=jnp.bfloat16
score_scale = HD ** (-0.5)
log2e = math.log2(math.e)
neg_big = -1e30

def dotf(a,b,ca,cb):
    return lax.dot_general(a,b,(((ca,),(cb,)),((),())),preferred_element_type=F32)

def place(blk_ref, r, BLK):
    b = blk_ref[r]
    return lax.div(b,2), pl.multiple_of(lax.rem(b,2)*BLK, BLK)

def causal_mask(S):
    return lax.broadcasted_iota(jnp.int32,(S,S),0) <= lax.broadcasted_iota(jnp.int32,(S,S),1)

def fwd_kernel(blk_ref, qkv_ref, mixed_ref, full_ref, lse_ref, q_s, k_s, v_s, o_s):
    nb, _, BLK = qkv_ref.shape
    ns = nb//2; S = 2*BLK
    def load(r, c):
        u, off = place(blk_ref, r, BLK)
        q_s[u, :, pl.ds(off,BLK)] = qkv_ref[r, 0:HD, :]
        v_s[u, :, pl.ds(off,BLK)] = qkv_ref[r, 2*HD:3*HD, :]
        k_s[u, pl.ds(off,BLK), :] = qkv_ref[r, HD:2*HD, :].astype(F32).T.astype(BF)
        return c
    lax.fori_loop(0, nb, load, 0)
    mult = score_scale*log2e
    def qstep(t, c):
        qT = q_s[t]
        def kv(u, carry, diag):
            m, l, acc = carry
            s = dotf(k_s[u], qT, 1, 0)
            if diag:
                s = jnp.where(causal_mask(S), s, neg_big)
            m_new = jnp.maximum(m, jnp.max(s, axis=0, keepdims=True))
            p = jnp.exp2(s*mult - m_new*mult)
            alpha = jnp.exp2((m-m_new)*mult)
            l = l*alpha + jnp.sum(p, axis=0, keepdims=True)
            acc = acc*alpha + dotf(v_s[u], p.astype(BF), 1, 0)
            return m_new, l, acc
        init = (jnp.full((1,S),neg_big,F32), jnp.zeros((1,S),F32), jnp.zeros((HD,S),F32))
        carry = lax.fori_loop(0, t, lambda u,cc: kv(u,cc,False), init)
        m, l, acc = kv(t, carry, True)
        o_s[t] = acc / l
        lse_ref[t] = m*mult + jnp.log2(l)
        return c
    lax.fori_loop(0, ns, qstep, 0)
    def put(r, c):
        u, off = place(blk_ref, r, BLK)
        o = o_s[u, :, pl.ds(off,BLK)]
        full_ref[r] = o
        mixed_ref[r] = o.astype(BF)
        return c
    lax.fori_loop(0, nb, put, 0)

def bwd_kernel(blk_ref, qkv_ref, do_ref, full_ref, lse_ref, dqkv_ref, q_s, k_s, v_s, g_s, kT_s, qn_s, gn_s, dq_s, dk_s, dv_s, dl_s):
    nb, _, BLK = qkv_ref.shape
    ns = nb//2; S = 2*BLK
    def load(r, c):
        u, off = place(blk_ref, r, BLK)
        q = qkv_ref[r, 0:HD, :]; k = qkv_ref[r, HD:2*HD, :]; v = qkv_ref[r, 2*HD:3*HD, :]; g = do_ref[r]
        q_s[u, :, pl.ds(off,BLK)] = q
        g_s[u, :, pl.ds(off,BLK)] = g
        kT_s[u, :, pl.ds(off,BLK)] = k
        k_s[u, pl.ds(off,BLK), :] = k.astype(F32).T.astype(BF)
        v_s[u, pl.ds(off,BLK), :] = v.astype(F32).T.astype(BF)
        qn_s[u, pl.ds(off,BLK), :] = q.astype(F32).T.astype(BF)
        gn_s[u, pl.ds(off,BLK), :] = g.astype(F32).T.astype(BF)
        dl_s[u, :, pl.ds(off,BLK)] = jnp.sum(g.astype(F32)*full_ref[r], axis=0, keepdims=True)
        return c
    lax.fori_loop(0, nb, load, 0)
    mult = score_scale*log2e
    def kvstep(i, c):
        u = ns-1-i
        k = k_s[u]; v = v_s[u]; kT = kT_s[u]
        def pair(t, diag):
            s = dotf(k, q_s[t], 1, 0)
            if diag:
                s = jnp.where(causal_mask(S), s, neg_big)
            p = jnp.exp2(s*mult - lse_ref[t])
            dp = dotf(v, g_s[t], 1, 0)
            ds = (p*(dp - dl_s[t])).astype(BF)
            dv = dotf(p.astype(BF), gn_s[t], 1, 0)
            dk = dotf(ds, qn_s[t], 1, 0)
            dq = dotf(kT, ds, 1, 0)
            return dq, dk, dv
        dq, dk, dv = pair(u, True)
        dq_s[u] = dq
        def step(t, carry):
            dk, dv = carry
            a, b, e = pair(t, False)
            dq_s[t] += a
            return dk+b, dv+e
        dk, dv = lax.fori_loop(u+1, ns, step, (dk, dv))
        dk_s[u] = dk; dv_s[u] = dv
        return c
    lax.fori_loop(0, ns, kvstep, 0)
    def put(r, c):
        u, off = place(blk_ref, r, BLK)
        dqkv_ref[r, 0:HD, :] = (dq_s[u, :, pl.ds(off,BLK)]*score_scale).astype(BF)
        dqkv_ref[r, HD:2*HD, :] = (dk_s[u, pl.ds(off,BLK), :]*score_scale).T.astype(BF)
        dqkv_ref[r, 2*HD:3*HD, :] = dv_s[u, pl.ds(off,BLK), :].T.astype(BF)
        return c
    lax.fori_loop(0, nb, put, 0)

VM = lambda: pl.BlockSpec(memory_space=pltpu.VMEM)
SM = lambda: pl.BlockSpec(memory_space=pltpu.SMEM)

def attend(blk, qkv):
    nb,_,BLK = qkv.shape; ns=nb//2; S=2*BLK
    sds=jax.ShapeDtypeStruct
    pairs = ns*(ns+1)//2
    return pl.pallas_call(fwd_kernel,
        out_shape=(sds((nb,HD,BLK),BF), sds((nb,HD,BLK),F32), sds((ns,1,S),F32)),
        in_specs=[SM(), VM()], out_specs=(VM(),VM(),VM()),
        scratch_shapes=[pltpu.VMEM((ns,HD,S),BF), pltpu.VMEM((ns,S,HD),BF), pltpu.VMEM((ns,HD,S),BF), pltpu.VMEM((ns,HD,S),F32)],
        compiler_params=pltpu.CompilerParams(vmem_limit_bytes=48*2**20),
        cost_estimate=pl.CostEstimate(flops=pairs*S*S*HD*4, bytes_accessed=nb*BLK*HD*12, transcendentals=pairs*S*S),
        name="attend_forward")(blk, qkv)

def attend_back(blk, qkv, do, full, lse):
    nb,_,BLK = qkv.shape; ns=nb//2; S=2*BLK
    pairs = ns*(ns+1)//2
    V=lambda s,d: pltpu.VMEM(s,d)
    return pl.pallas_call(bwd_kernel,
        out_shape=jax.ShapeDtypeStruct((nb,3*HD,BLK),BF),
        in_specs=[SM(), VM(), VM(), VM(), VM()], out_specs=VM(),
        scratch_shapes=[V((ns,HD,S),BF), V((ns,S,HD),BF), V((ns,S,HD),BF), V((ns,HD,S),BF), V((ns,HD,S),BF), V((ns,S,HD),BF), V((ns,S,HD),BF),
          V((ns,HD,S),F32), V((ns,S,HD),F32), V((ns,S,HD),F32), V((ns,1,S),F32)],
        compiler_params=pltpu.CompilerParams(vmem_limit_bytes=56*2**20),
        cost_estimate=pl.CostEstimate(flops=pairs*S*S*HD*10, bytes_accessed=nb*BLK*HD*18, transcendentals=pairs*S*S),
        name="attend_backward")(blk, qkv, do, full, lse)


def rotary_rows(where_at):
    half_dims = ROT // 2
    frequency = rope_base ** (-(jnp.arange(half_dims, dtype=jnp.float32) * 2.0) / ROT)
    angles = frequency[:, None] * where_at.astype(jnp.float32)[None, :]
    return (jnp.cos(angles), jnp.sin(angles))


def turn(columns, cosine, sine_part):
    half_dims = ROT // 2
    first_half = columns[:, :half_dims]
    second = columns[:, half_dims:ROT]
    return jnp.concatenate(
        [
            first_half * cosine - second * sine_part,
            second * cosine + first_half * sine_part,
            columns[:, ROT:],
        ],
        axis=1,
    )


def exchange(values):
    return lax.all_to_all(values, "ctx", split_axis=0, concat_axis=0, tiled=True)


def blocks_out(columns, blocks):
    parts, heads, _, rows = columns.shape
    split = columns.reshape(parts, heads, HD, blocks, rows // blocks)
    return jnp.transpose(split, (1, 3, 0, 2, 4)).reshape(heads, blocks, parts * HD, rows // blocks)


def blocks_in(arrived, parts):
    heads, blocks, _, block_rows = arrived.shape
    split = arrived.reshape(heads, blocks, parts, HD, block_rows)
    return jnp.transpose(split, (2, 0, 3, 1, 4)).reshape(parts, heads, HD, blocks * block_rows)


def by_head_forward(turned, positions, contexts):
    rows = turned.shape[-1]
    block_rows = rows // 2
    block_ids = positions[::block_rows] // block_rows
    arrived = exchange(blocks_out(turned, 2)).reshape(2 * contexts, 3 * HD, block_rows)
    mixed, full, lse = attend(block_ids, arrived)
    back = exchange(mixed.reshape(contexts, 2, HD, block_rows))
    mixed_columns = blocks_in(back, 1).reshape(-1, rows)
    return mixed_columns, (block_ids, arrived, full, lse)


def by_head_backward(d_mixed, kept):
    block_ids, arrived, full, lse = kept
    heads = d_mixed.shape[0] // HD
    rows = d_mixed.shape[1]
    sent = exchange(blocks_out(d_mixed.reshape(1, heads, HD, rows), 2))
    grads = attend_back(block_ids, arrived, sent.reshape(full.shape), full, lse)
    back = exchange(grads.reshape(heads, 2, 3 * HD, rows // 2))
    return blocks_in(back, 3)


def by_rows_forward(turned, positions, row_pos):
    heads_here, rows = turned.shape[1], turned.shape[3]
    half_rows = rows // 2
    rows_first = jnp.transpose(turned, (0, 3, 1, 2))
    query_heads = rows_first[0]
    head_key = rows_first[1].reshape(rows, heads_here * HD)
    head_value = rows_first[2].reshape(rows, heads_here * HD)
    pos_halves = (row_pos[:half_rows], row_pos[half_rows:])
    query_halves = (query_heads[:half_rows], query_heads[half_rows:])
    start_state = (
        jnp.full((heads_here, half_rows), masked_score, jnp.float32),
        jnp.zeros((heads_here, half_rows), jnp.float32),
        jnp.zeros((heads_here, half_rows, HD), jnp.float32),
    )
    attend_fns = (
        partial(attend_block, query_halves[0], pos_halves[0]),
        partial(attend_block, query_halves[1], pos_halves[1]),
    )
    states = query_side_fold(
        attend_fns,
        pos_halves,
        positions,
        rows,
        (start_state, start_state),
        (
            lax.all_gather(head_key, "ctx", axis=0, tiled=True),
            lax.all_gather(head_value, "ctx", axis=0, tiled=True),
        ),
    )
    lse_halves = (states[0][0] + jnp.log(states[0][1]), states[1][0] + jnp.log(states[1][1]))
    attended = jnp.concatenate(
        [states[0][2] / states[0][1][..., None], states[1][2] / states[1][1][..., None]], axis=1
    )
    mixed_columns = jnp.transpose(attended, (0, 2, 1)).reshape(heads_here * HD, rows)
    kept = (query_halves, pos_halves, head_key, head_value, lse_halves, attended)
    return mixed_columns.astype(jnp.bfloat16), kept


def by_rows_backward(d_mixed, positions, kept, contexts):
    query_halves, pos_halves, head_key, head_value, lse_halves, attended = kept
    heads_here, rows, _ = attended.shape
    half_rows = rows // 2
    grad_heads = jnp.transpose(d_mixed.reshape(heads_here, HD, rows), (2, 0, 1))
    row_delta = jnp.sum(
        jnp.transpose(grad_heads.astype(jnp.float32), (1, 0, 2)) * attended, axis=-1
    )
    grad_halves = (grad_heads[:half_rows], grad_heads[half_rows:])
    delta_halves = (row_delta[:, :half_rows], row_delta[:, half_rows:])
    zero_query = jnp.zeros((heads_here, half_rows, HD), jnp.float32)
    zero_keys = jnp.zeros((rows * contexts, heads_here * HD), jnp.float32)
    query_grads, key_grads, value_grads = backward_fold(
        query_halves,
        pos_halves,
        grad_halves,
        lse_halves,
        delta_halves,
        positions,
        rows,
        ((zero_query, zero_query), zero_keys, zero_keys),
        (
            lax.all_gather(head_key, "ctx", axis=0, tiled=True),
            lax.all_gather(head_value, "ctx", axis=0, tiled=True),
        ),
    )
    query_columns = jnp.transpose(jnp.concatenate(query_grads, axis=1), (0, 2, 1))

    def own_columns(grads):
        own = lax.psum_scatter(grads, "ctx", scatter_dimension=0, tiled=True)
        return jnp.transpose(own.reshape(rows, heads_here, HD), (1, 2, 0))

    columns = jnp.stack([query_columns, own_columns(key_grads), own_columns(value_grads)])
    return columns.astype(jnp.bfloat16)


def gather_tokens(values):
    return lax.all_gather(values, "fsdp", axis=0, tiled=True)


def scatter_tokens(partial_rows):
    summed = lax.psum_scatter(
        partial_rows.astype(jnp.bfloat16), "fsdp", scatter_dimension=0, tiled=True
    )
    return summed.astype(jnp.float32)


def scatter_grad(grad_value, dimension):
    summed = lax.psum_scatter(
        grad_value.astype(jnp.bfloat16), "ctx", scatter_dimension=dimension, tiled=True
    )
    return summed.astype(jnp.float32)


def gather_small(gain_one, shift_one, gain_two, shift_two, bias):
    width = gain_one.shape[0]
    packed = jnp.concatenate([gain_one, shift_one, gain_two, shift_two, bias.reshape(-1)])
    whole = lax.all_gather(packed.astype(jnp.bfloat16), "ctx", axis=0, tiled=False)
    vectors = [
        whole[:, index * width : (index + 1) * width].reshape(-1).astype(jnp.float32)
        for index in range(4)
    ]
    parts = whole[:, 4 * width :].reshape((-1,) + bias.shape)
    columns = jnp.transpose(parts, (1, 2, 0, 3)).reshape(3, bias.shape[1], HD)
    return vectors + [columns.astype(jnp.float32)]


def local(
    inputs,
    cotangent,
    positions,
    gain_attention,
    shift_attention,
    weight_project,
    bias_project,
    weight_output,
    gain_feedforward,
    shift_feedforward,
    weight_gateup,
    weight_down,
    momentum_gain_attention,
    momentum_shift_attention,
    momentum_weight_project,
    momentum_bias_project,
    momentum_weight_output,
    momentum_gain_feedforward,
    momentum_shift_feedforward,
    momentum_weight_gateup,
    momentum_weight_down,
    variance_gain_attention,
    variance_shift_attention,
    variance_weight_project,
    variance_bias_project,
    variance_weight_output,
    variance_gain_feedforward,
    variance_shift_feedforward,
    variance_weight_gateup,
    variance_weight_down,
):
    tokens = inputs.shape[0]
    groups = lax.axis_size("fsdp")
    contexts = lax.axis_size("ctx")
    heads_here = H // groups
    row_count = tokens * groups
    spread_heads = heads_here == contexts
    row_pos = lax.dynamic_slice_in_dim(positions, lax.axis_index("ctx") * row_count, row_count)
    cosine, sine_part = rotary_rows(row_pos)
    gain_one, shift_one, gain_two, shift_two, group_bias = gather_small(
        gain_attention, shift_attention, gain_feedforward, shift_feedforward, bias_project
    )
    group_project = lax.all_gather(weight_project.astype(jnp.bfloat16), "ctx", axis=0, tiled=True)
    group_output = lax.all_gather(weight_output.astype(jnp.bfloat16), "ctx", axis=1, tiled=True)
    group_gateup = lax.all_gather(weight_gateup.astype(jnp.bfloat16), "ctx", axis=0, tiled=True)
    group_down = lax.all_gather(weight_down.astype(jnp.bfloat16), "ctx", axis=1, tiled=True)
    normed_one, inverse_one = norm_parts(inputs)
    first_act = gather_tokens((normed_one * gain_one + shift_one).astype(jnp.bfloat16))
    d_branch = gather_tokens(cotangent.astype(jnp.bfloat16))
    projected = (
        jnp.einsum("dge,td->get", group_project, first_act, preferred_element_type=jnp.float32)
        .reshape(3, heads_here, HD, row_count)
        + group_bias[..., None]
    )
    turned = jnp.stack(
        [
            turn(projected[0], cosine, sine_part),
            turn(projected[1], cosine, sine_part),
            projected[2],
        ]
    ).astype(jnp.bfloat16)
    if spread_heads:
        mixed, kept = by_head_forward(turned, positions, contexts)
    else:
        mixed, kept = by_rows_forward(turned, positions, row_pos)
    middle = inputs + scatter_tokens(
        jnp.einsum("et,ed->td", mixed, group_output, preferred_element_type=jnp.float32)
    )
    normed_two, inverse_two = norm_parts(middle)
    second_act = gather_tokens((normed_two * gain_two + shift_two).astype(jnp.bfloat16))
    gate_part = jnp.dot(second_act, group_gateup[:, 0], preferred_element_type=jnp.float32)
    up_part = jnp.dot(second_act, group_gateup[:, 1], preferred_element_type=jnp.float32)
    hidden = (jax.nn.silu(gate_part) * up_part).astype(jnp.bfloat16)
    output = middle + scatter_tokens(
        jnp.dot(hidden, group_down, preferred_element_type=jnp.float32)
    )
    grad_down = jnp.einsum("tu,td->ud", hidden, d_branch, preferred_element_type=jnp.float32)
    d_hidden = jnp.einsum("td,ud->tu", d_branch, group_down, preferred_element_type=jnp.float32)
    gate_sigmoid = jax.nn.sigmoid(gate_part)
    d_gate = d_hidden * up_part * gate_sigmoid * (1.0 + gate_part * (1.0 - gate_sigmoid))
    d_up = d_hidden * jax.nn.silu(gate_part)
    d_gate_up = jnp.stack([d_gate, d_up], axis=0).astype(jnp.bfloat16)
    grad_gateup = jnp.einsum(
        "td,gtu->dgu", second_act, d_gate_up, preferred_element_type=jnp.float32
    )
    d_second = scatter_tokens(
        jnp.einsum("gtu,dgu->td", d_gate_up, group_gateup, preferred_element_type=jnp.float32)
    )
    d_middle = cotangent + norm_back(d_second, normed_two, inverse_two, gain_two)
    d_attend = gather_tokens(d_middle.astype(jnp.bfloat16))
    grad_output = jnp.einsum("et,td->ed", mixed, d_attend, preferred_element_type=jnp.float32)
    d_mixed = jnp.einsum(
        "ed,td->et", group_output, d_attend, preferred_element_type=jnp.float32
    ).astype(jnp.bfloat16)
    if spread_heads:
        columns = by_head_backward(d_mixed, kept)
    else:
        columns = by_rows_backward(d_mixed, positions, kept, contexts)
    columns = columns.astype(jnp.float32)
    d_projected = jnp.stack(
        [
            turn(columns[0], cosine, -sine_part),
            turn(columns[1], cosine, -sine_part),
            columns[2],
        ]
    ).astype(jnp.bfloat16)
    grad_bias = jnp.sum(d_projected.astype(jnp.float32), axis=-1)
    d_flat = d_projected.reshape(3, heads_here * HD, row_count)
    grad_project = jnp.einsum(
        "td,get->dge", first_act, d_flat, preferred_element_type=jnp.float32
    )
    d_first = scatter_tokens(
        jnp.einsum("get,dge->td", d_flat, group_project, preferred_element_type=jnp.float32)
    )
    input_grad = d_middle + norm_back(d_first, normed_one, inverse_one, gain_one)
    vector_grads = lax.psum(
        jnp.stack(
            [
                jnp.sum(d_first * normed_one, axis=0),
                jnp.sum(d_first, axis=0),
                jnp.sum(d_second * normed_two, axis=0),
                jnp.sum(d_second, axis=0),
            ]
        ),
        ("ctx", "fsdp"),
    )
    width = gain_attention.shape[0]
    own_vectors = lax.dynamic_slice_in_dim(
        vector_grads, lax.axis_index("ctx") * width, width, axis=1
    )
    gradients = [
        own_vectors[0],
        own_vectors[1],
        scatter_grad(grad_project, 0),
        lax.psum_scatter(grad_bias, "ctx", scatter_dimension=2, tiled=True),
        scatter_grad(grad_output, 1),
        own_vectors[2],
        own_vectors[3],
        scatter_grad(grad_gateup, 0),
        scatter_grad(grad_down, 1),
    ]
    params = [
        gain_attention,
        shift_attention,
        weight_project,
        bias_project,
        weight_output,
        gain_feedforward,
        shift_feedforward,
        weight_gateup,
        weight_down,
    ]
    momenta = [
        momentum_gain_attention,
        momentum_shift_attention,
        momentum_weight_project,
        momentum_bias_project,
        momentum_weight_output,
        momentum_gain_feedforward,
        momentum_shift_feedforward,
        momentum_weight_gateup,
        momentum_weight_down,
    ]
    variances = [
        variance_gain_attention,
        variance_shift_attention,
        variance_weight_project,
        variance_bias_project,
        variance_weight_output,
        variance_gain_feedforward,
        variance_shift_feedforward,
        variance_weight_gateup,
        variance_weight_down,
    ]
    new_params = []
    new_momenta = []
    new_variances = []
    for index in range(9):
        new_value, moment, second_moment = adam_update(
            params[index], gradients[index], momenta[index], variances[index]
        )
        new_params.append(new_value)
        new_momenta.append(moment)
        new_variances.append(second_moment)
    new_params[0] = new_params[0] - params[0]
    new_params[5] = new_params[5] - params[5]
    return tuple([output, input_grad] + gradients + new_params + new_momenta + new_variances)


def solution(mesh):
    in_specs = (
        P(("ctx", "fsdp"), None),
        P(("ctx", "fsdp"), None),
        P(),
        P("ctx"),
        P("ctx"),
        P("ctx", None, "fsdp"),
        P(None, "fsdp", "ctx"),
        P("fsdp", "ctx"),
        P("ctx"),
        P("ctx"),
        P("ctx", None, "fsdp"),
        P("fsdp", "ctx"),
        P("ctx"),
        P("ctx"),
        P("ctx", None, "fsdp"),
        P(None, "fsdp", "ctx"),
        P("fsdp", "ctx"),
        P("ctx"),
        P("ctx"),
        P("ctx", None, "fsdp"),
        P("fsdp", "ctx"),
        P("ctx"),
        P("ctx"),
        P("ctx", None, "fsdp"),
        P(None, "fsdp", "ctx"),
        P("fsdp", "ctx"),
        P("ctx"),
        P("ctx"),
        P("ctx", None, "fsdp"),
        P("fsdp", "ctx"),
    )
    out_specs = (
        P(("ctx", "fsdp"), None),
        P(("ctx", "fsdp"), None),
        P("ctx"),
        P("ctx"),
        P("ctx", None, "fsdp"),
        P(None, "fsdp", "ctx"),
        P("fsdp", "ctx"),
        P("ctx"),
        P("ctx"),
        P("ctx", None, "fsdp"),
        P("fsdp", "ctx"),
        P("ctx"),
        P("ctx"),
        P("ctx", None, "fsdp"),
        P(None, "fsdp", "ctx"),
        P("fsdp", "ctx"),
        P("ctx"),
        P("ctx"),
        P("ctx", None, "fsdp"),
        P("fsdp", "ctx"),
        P("ctx"),
        P("ctx"),
        P("ctx", None, "fsdp"),
        P(None, "fsdp", "ctx"),
        P("fsdp", "ctx"),
        P("ctx"),
        P("ctx"),
        P("ctx", None, "fsdp"),
        P("fsdp", "ctx"),
        P("ctx"),
        P("ctx"),
        P("ctx", None, "fsdp"),
        P(None, "fsdp", "ctx"),
        P("fsdp", "ctx"),
        P("ctx"),
        P("ctx"),
        P("ctx", None, "fsdp"),
        P("fsdp", "ctx"),
    )
    return jax.shard_map(local, mesh=mesh, in_specs=in_specs, out_specs=out_specs, check_vma=False)
```
